32 devices in a mesh: groups: 2 (over x), cube: 16 (over z, y, core).
Axes of the slice: x: 2, y: 2, z: 4, core: 2. Of those that a mesh axis runs over, the one named last changes fastest.
Arguments:
- patches: float32 [1024, 128, 128], P(('groups', 'cube')), parts along dimension 0, may hold values from -6 to 6
- ghost_rows: float32 [1024, 2, 128], P(('groups', 'cube')), parts along dimension 0, may hold values from -6 to 6
- courant: float32 [1024, 2], P(('groups', 'cube')), parts along dimension 0, may hold values from 0.2 to 0.48
- patch_ids: int32 [1024], P(('groups', 'cube')), parts along dimension 0, may hold values from 0 to 511, each once
- initial_load: int32 [32], P(('groups', 'cube')), parts along dimension 0, may hold values from 0 to 32, as said below
- flow_counts: int32 [3, 32, 4], P(None, ('groups', 'cube')), parts along dimension 1, may hold values from 0 to 8, as said below
Outputs:
- advected: float32 [1024, 128, 128], P(('groups', 'cube')), parts along dimension 0
- final_ids: int32 [1024], P(('groups', 'cube')), parts along dimension 0
- imbalance: float32 [6], P('groups'), parts along dimension 0
The draws below stay inside these ranges and needn't reach their ends.
There are 2 independent parts, one for each index of `groups`. The reference program is written for one: setup_inputs(seed, part) draws one part's arguments, and reference() takes and returns one part's arrays. A program takes and returns all parts, laid end to end along the dimension named above; each array names one. Nothing has to cross between parts.
Inputs may be any that keep to these rules, and one draw needn't show every extreme that they name: For some even k drawn from the seed, initial_load[k] = 32 and initial_load[k + 1] = 0. `flow_counts`: of two partners along a dimension at most one sends; a device never sends more than it holds and never holds more than 32. Counts of sweep 0 are at most 8 (reached in every draw), counts of later sweeps at most 4. At no time does a device hold more than 8 records that started on one other device; after the sweeps some device holds exactly 8 records that started on one other device.
All inputs are finite; a program needn't handle non-finite values.
Results may differ from the reference program's by a relative error of at most 0.0003.
Values sent between devices are 32-bit elements; how exact they have to be, the bound alone decides.
A program may use at most 64 MiB of HBM per device.

```python
from functools import partial
import jax
import jax.numpy as jnp
from jax import lax

PATCH = 128
SLOTS = 32
SWEEPS = 3
LOGC = 4
N_CUBE = 16


def cut_rows_drawn(source, first_free, capacity):
    padded = jnp.concatenate([source, jnp.zeros((capacity,) + source.shape[1:], source.dtype)], 0)
    return lax.dynamic_slice_in_dim(padded, first_free, capacity, 0)


def place_rows_drawn(source, spare_rows, first_free, incoming, capacity):
    slot_count = source.shape[0]
    row_index = jnp.arange(slot_count, dtype=jnp.int32)
    retained = jnp.where(row_index < first_free, source, jnp.zeros_like(source))
    extra_index = jnp.arange(capacity, dtype=jnp.int32)
    landed = jnp.where(extra_index < incoming, spare_rows, jnp.zeros_like(spare_rows))
    padded = jnp.concatenate([retained, jnp.zeros((capacity,), source.dtype)], 0)
    return lax.dynamic_update_slice_in_dim(padded, landed, first_free, 0)[:slot_count]


def evolve(key):
    seeded = jax.random.fold_in(key, 11)
    first_key, second_key = jax.random.split(seeded)
    loading = jax.random.randint(first_key, (N_CUBE,), 0, SLOTS + 1).astype(jnp.int32)
    chosen = (jax.random.randint(second_key, (), 0, N_CUBE // 2) * 2).astype(jnp.int32)
    loading = loading.at[chosen].set(SLOTS).at[chosen + 1].set(0)
    initial = loading
    device_index = jnp.arange(N_CUBE, dtype=jnp.int32)
    slot_index = jnp.arange(SLOTS, dtype=jnp.int32)
    bound = SLOTS // 4
    anchor = jnp.where(slot_index[None, :] < loading[:, None], device_index[:, None] + 1, 0).astype(jnp.int32)
    sweeps_out = []
    for sweep_no in range(SWEEPS):
        limit = SLOTS // 4 if sweep_no == 0 else SLOTS // 8
        per_dim = []
        for dim_no in range(LOGC):
            partner = jnp.bitwise_xor(device_index, 1 << dim_no)
            proposed = jnp.clip((loading - loading[partner]) // 4, 0, limit).astype(jnp.int32)
            proposed = jnp.where(device_index == chosen + 1, 0, proposed).astype(jnp.int32)
            tail_index = jnp.arange(limit, dtype=jnp.int32)
            position = loading[:, None] - 1 - tail_index[None, :]
            tail = jnp.take_along_axis(anchor, jnp.clip(position, 0, SLOTS - 1), 1)
            tail = jnp.where(position >= 0, tail, 0)
            onehot = (tail[:, :, None] == device_index[None, None, :] + 1).astype(jnp.int32)
            running = jnp.cumsum(onehot, 1)
            held = jnp.sum((anchor[:, :, None] == device_index[None, None, :] + 1).astype(jnp.int32), 1)
            partner_held = held[partner]
            others = device_index[None, :] != partner[:, None]
            fits = (partner_held[:, None, :] + running <= bound) | jnp.logical_not(others[:, None, :])
            allowed = jnp.all(fits, 2).astype(jnp.int32)
            good = jnp.sum(jnp.cumprod(allowed, 1), 1).astype(jnp.int32)
            outgoing = jnp.minimum(proposed, good).astype(jnp.int32)
            first_free = loading - outgoing
            incoming = outgoing[partner]
            outbox = jax.vmap(partial(cut_rows_drawn, capacity=bound))(anchor, first_free)
            anchor = jax.vmap(partial(place_rows_drawn, capacity=bound))(anchor, outbox[partner], first_free, incoming)
            loading = first_free + incoming
            per_dim.append(outgoing)
        sweeps_out.append(jnp.stack(per_dim, 1))
    return (initial, jnp.stack(sweeps_out, 0).astype(jnp.int32))


def draw_initial_load(key, part):
    return evolve(key)[0]


def draw_flow_counts(key, part):
    return evolve(key)[1]


def block_scale(rng, dims, pieces, smallest, top_value):
    factor_of = 1.0
    for dim, parts in pieces:
        draws = jax.random.uniform(jax.random.fold_in(jax.random.fold_in(rng, 6), dim), (parts,), jnp.float32, smallest / len(pieces), top_value / len(pieces))
        factor_of = factor_of * jnp.repeat(jnp.exp(draws), dims[dim] // parts).reshape((-1,) + (1,) * (len(dims) - 1 - dim))
    return factor_of


def gaussian(own_key, shape, scale, reach, shards=(), kind=jnp.bfloat16):
    drawn = jax.random.normal(own_key, shape, jnp.float32) * scale
    if len(shards) > 0:
        drawn = block_scale(own_key, shape, shards, -0.22, 0.18) * drawn
    return jnp.clip(drawn, min=-reach, max=reach).astype(kind)


def setup_inputs(seed: int = 0, part: int = 0) -> dict:
    key_list = jax.random.split(jax.random.key(seed), 7)
    part_keys = jax.random.split(jax.random.fold_in(key_list[6], part), 7)
    return {
        "patches": gaussian(part_keys[0], (N_CUBE * SLOTS, PATCH, PATCH), 1.0, 6.0, ((0, 16),), jnp.float32),
        "ghost_rows": gaussian(part_keys[1], (N_CUBE * SLOTS, 2, PATCH), 1.0, 6.0, ((0, 16),), jnp.float32),
        "courant": jnp.clip(0.2 + 0.279999986 * jax.random.uniform(part_keys[2], (N_CUBE * SLOTS, 2), jnp.float32) ** block_scale(part_keys[2], (N_CUBE * SLOTS, 2), ((0, 16),), -0.2, 0.2), 0.2, 0.48),
        "patch_ids": jax.random.permutation(part_keys[3], N_CUBE * SLOTS).astype(jnp.int32),
        "initial_load": draw_initial_load(jax.random.fold_in(jax.random.fold_in(key_list[6], part), 71), part),
        "flow_counts": draw_flow_counts(jax.random.fold_in(jax.random.fold_in(key_list[6], part), 71), part),
    }


def cut_rows(source, first_free, capacity):
    padded = jnp.concatenate([source, jnp.zeros((capacity,) + source.shape[1:], source.dtype)], 0)
    return lax.dynamic_slice_in_dim(padded, first_free, capacity, 0)


def place_rows(source, spare_rows, first_free, incoming, capacity):
    slot_count = source.shape[0]
    shape_tail = (1,) * (source.ndim - 1)
    row_index = jnp.arange(slot_count, dtype=jnp.int32).reshape((slot_count,) + shape_tail)
    retained = jnp.where(row_index < first_free, source, jnp.zeros_like(source))
    extra_index = jnp.arange(capacity, dtype=jnp.int32).reshape((capacity,) + shape_tail)
    landed = jnp.where(extra_index < incoming, spare_rows, jnp.zeros_like(spare_rows))
    padded = jnp.concatenate([retained, jnp.zeros((capacity,) + source.shape[1:], source.dtype)], 0)
    return lax.dynamic_update_slice_in_dim(padded, landed, first_free, 0)[:slot_count]


def advect(field, ghost_rows, courant, holding):
    western = jnp.concatenate([ghost_rows[:, 1, :][:, :, None], field[:, :, :-1]], 2)
    northern = jnp.concatenate([ghost_rows[:, 0, :][:, None, :], field[:, :-1, :]], 1)
    along_x = courant[:, 0][:, None, None]
    along_y = courant[:, 1][:, None, None]
    stepped = field - along_x * (field - western) - along_y * (field - northern)
    row_index = jnp.arange(field.shape[0], dtype=jnp.int32)[:, None, None]
    return jnp.where(row_index < holding, stepped, jnp.zeros_like(stepped))


def reference(patches, ghost_rows, courant, patch_ids, initial_load, flow_counts):
    resident = [patches.reshape(N_CUBE, SLOTS, PATCH, PATCH), ghost_rows.reshape(N_CUBE, SLOTS, 2, PATCH),
                courant.reshape(N_CUBE, SLOTS, 2), patch_ids.reshape(N_CUBE, SLOTS)]
    holding = initial_load.astype(jnp.int32)
    device_index = jnp.arange(N_CUBE, dtype=jnp.int32)
    capacity = SLOTS // 4
    peak_loads = []
    for sweep_no in range(SWEEPS):
        for dim_no in range(LOGC):
            outgoing = flow_counts[sweep_no, :, dim_no]
            partner = jnp.bitwise_xor(device_index, 1 << dim_no)
            first_free = holding - outgoing
            incoming = outgoing[partner]
            cutter = jax.vmap(partial(cut_rows, capacity=capacity))
            placer = jax.vmap(partial(place_rows, capacity=capacity))
            outbox = [cutter(source, first_free) for source in resident]
            resident = [placer(source, sent[partner], first_free, incoming) for source, sent in zip(resident, outbox)]
            holding = first_free + incoming
        peak_loads.append(jnp.max(holding).astype(jnp.float32))
    total_load = jnp.sum(initial_load.astype(jnp.float32))
    imbalance = jnp.stack(peak_loads) * float(N_CUBE) / total_load
    advected = jax.vmap(advect)(resident[0], resident[1], resident[2], holding)
    row_index = jnp.arange(SLOTS, dtype=jnp.int32)[None, :]
    final_ids = jnp.where(row_index < holding[:, None], resident[3], -1)
    return advected.reshape(N_CUBE * SLOTS, PATCH, PATCH), final_ids.reshape(N_CUBE * SLOTS), imbalance
```

```python
import functools

import jax
import jax.numpy as jnp
from jax import lax
from jax.experimental import pallas as pl
from jax.experimental.pallas import tpu as pltpu
from jax.sharding import PartitionSpec as P

SWEEPS = 3
CUBE = "cube"
GROUPS = "groups"


def capacity_classes(dims, slots):
    full = [slots * 2 ** min(b, dims - 1 - b) for b in range(dims)]
    plans = []
    for first, rest in ((8, 4), (10, 6), (12, 8), (16, 12)):
        plans.append(tuple(min(f, first if b == 0 else rest) for b, f in enumerate(full)))
    plans.append(tuple(full))
    return plans


def partner_rows(value, bit, index):
    size = value.shape[0]
    up = pltpu.roll(value, 2**bit, axis=0)
    down = pltpu.roll(value, size - 2**bit, axis=0)
    return jnp.where(((index >> bit) & 1) == 1, up, down)


def track(meta, cube, dims, slots):
    records = cube * slots
    wide = (cube, 128)
    row = lax.broadcasted_iota(jnp.int32, wide, 0)
    device = lax.broadcasted_iota(jnp.int32, (cube, records), 0)
    index = lax.broadcasted_iota(jnp.int32, (1, records), 1)
    origin, start = index // slots, index % slots
    load = jnp.broadcast_to(meta[:, 0:1], wide)

    def look_up(where, column):
        picked = jnp.where(device == where, jnp.broadcast_to(column[:, 0:1], device.shape), 0)
        return jnp.sum(picked, axis=0, keepdims=True)

    occupied = start < look_up(origin, load)
    at, pos = origin, start
    peaks = []
    for sweep in range(SWEEPS):
        for bit in range(dims):
            column = 1 + sweep * dims + bit
            count = jnp.broadcast_to(meta[:, column : column + 1], wide)
            free = load - count
            shift = partner_rows(free, bit, row) - free
            moves = occupied & (pos >= look_up(at, free))
            pos = pos + jnp.where(moves, look_up(at, shift), 0)
            at = jnp.where(moves, at ^ (2**bit), at)
            load = free + partner_rows(count, bit, row)
        peaks.append(jnp.max(load))
    total = jnp.sum(meta[:, 0:1].astype(jnp.float32))
    crossing = []
    for bit in range(dims):
        low = 2**bit - 1
        current = (at & low) | (origin & ~low)
        mover = occupied & ((((origin ^ at) >> bit) & 1) == 1)
        current = jnp.where(mover, current, -1)
        crossing.append((current, (device == current).astype(jnp.float32)))
    needs = [jnp.max(jnp.sum(hot, axis=1, keepdims=True)).astype(jnp.int32) for _, hot in crossing]
    return occupied, at, pos, load, start, peaks, total, crossing, needs


def plan_kernel(groups, cube, dims, slots, plans, width, meta_ref, ids_ref, tab_ref, word_ref, ids_out_ref, imb_ref):
    me, group = lax.axis_index(CUBE), lax.axis_index(GROUPS)
    records = cube * slots
    meta = meta_ref[pl.ds(pl.multiple_of(group * cube, cube), cube), :]
    occupied, at, pos, load, start, peaks, total, crossing, needs = track(meta, cube, dims, slots)
    for other in range(1, groups):
        there = lax.rem(group + other, groups)
        block = meta_ref[pl.ds(pl.multiple_of(there * cube, cube), cube), :]
        more = track(block, cube, dims, slots)[-1]
        needs = [jnp.maximum(a, b) for a, b in zip(needs, more)]
    choice = jnp.int32(len(plans) - 1)
    for k in reversed(range(len(plans) - 1)):
        fits = needs[0] <= plans[k][0]
        for b in range(1, dims):
            fits = fits & (needs[b] <= plans[k][b])
        choice = jnp.where(fits, k, choice)
    bases = []
    for b in range(dims):
        base = jnp.int32(0)
        for k, plan in enumerate(plans):
            base = jnp.where(choice == k, slots + sum(plan[:b]), base)
        bases.append(base)

    hot = jnp.concatenate([h for _, h in crossing], axis=0).astype(jnp.bfloat16)
    before = lax.broadcasted_iota(jnp.int32, (records, records), 0) < lax.broadcasted_iota(
        jnp.int32, (records, records), 1
    )
    ranks = jnp.dot(hot, before.astype(jnp.bfloat16), preferred_element_type=jnp.float32)
    slot = start
    rows, keys = [], []
    column = lax.broadcasted_iota(jnp.int32, (width, records), 0)
    for b in range(dims):
        current, own = crossing[b]
        rank = jnp.sum(own * ranks[b * cube : (b + 1) * cube], axis=0, keepdims=True).astype(jnp.int32)
        rows.append(slot)
        keys.append((column == jnp.where(current == me, rank, -1)).astype(jnp.float32))
        slot = jnp.where(current >= 0, bases[b] + rank, slot)
    rows += [slot, ids_ref[pl.ds(group, 1), :]]
    column = lax.broadcasted_iota(jnp.int32, (128, records), 0)
    keys.append((column == jnp.where(occupied & (at == me), pos, -1)).astype(jnp.float32))
    rows += [jnp.zeros((1, records), jnp.int32)] * (8 - len(rows))
    left = jnp.concatenate(rows, axis=0).astype(jnp.float32)
    right = jnp.concatenate(keys, axis=0)
    table = lax.dot_general(
        left, right, (((1,), (1,)), ((), ())),
        precision=lax.Precision.HIGHEST, preferred_element_type=jnp.float32,
    ).astype(jnp.int32)
    tab_ref[...] = table
    mine = lax.broadcasted_iota(jnp.int32, load.shape, 0) == me
    held = jnp.sum(jnp.where(mine, load, 0), axis=0, keepdims=True)
    lane = lax.broadcasted_iota(jnp.int32, (1, 128), 1)
    ids_out_ref[...] = jnp.where(lane < held, table[dims + 1 : dims + 2, dims * width : dims * width + 128], -1)
    word_ref[0] = choice
    word_ref[1] = jnp.max(held)
    peak = jnp.zeros((1, 128), jnp.float32)
    for sweep in range(SWEEPS):
        peak = jnp.where(lane == sweep, peaks[sweep].astype(jnp.float32), peak)
    imb_ref[...] = peak * float(cube) / total


def move_kernel(caps, slots, width, tab_ref, word_ref, adv_ref, out_ref, main, *scratch):
    dims = len(caps)
    outbox, recvs = scratch[0], scratch[1 : 1 + dims]
    send_sem, recv_sem, load_sem = scratch[1 + dims :]
    me = lax.axis_index(CUBE)
    partners = [me + 2**b - 2 * 2**b * ((me // 2**b) % 2) for b in range(dims)]
    fetch = pltpu.make_async_copy(adv_ref, main.at[pl.ds(0, slots)], load_sem)
    fetch.start()
    barrier = pltpu.get_barrier_semaphore()
    for p in partners:
        pl.semaphore_signal(barrier, inc=1, device_id={CUBE: p}, device_id_type=pl.DeviceIdType.MESH)
    pl.semaphore_wait(barrier, dims)
    fetch.wait()
    base = slots
    for b in range(dims):
        send, recv = outbox.at[pl.ds(0, caps[b])], recvs[b]

        def pack(j, carry):
            send[j] = main[tab_ref[b, b * width + j]]
            return carry

        lax.fori_loop(0, caps[b], pack, 0)
        copy = pltpu.make_async_remote_copy(
            src_ref=send, dst_ref=recv, send_sem=send_sem.at[b], recv_sem=recv_sem.at[b],
            device_id={CUBE: partners[b]}, device_id_type=pl.DeviceIdType.MESH,
        )
        copy.start()
        copy.wait()

        def keep(j, carry):
            main[base + j] = recv[j]
            return carry

        lax.fori_loop(0, caps[b], keep, 0)
        base += caps[b]

    held = word_ref[1]

    def place(j, carry):
        out_ref[j] = jnp.where(j < held, main[tab_ref[dims, dims * width + j]], 0.0)
        return carry

    lax.fori_loop(0, slots, place, 0)


def advect(field, ghost_rows, courant):
    western = jnp.concatenate([ghost_rows[:, 1, :][:, :, None], field[:, :, :-1]], 2)
    northern = jnp.concatenate([ghost_rows[:, 0, :][:, None, :], field[:, :-1, :]], 1)
    along_x = courant[:, 0][:, None, None]
    along_y = courant[:, 1][:, None, None]
    return field - along_x * (field - western) - along_y * (field - northern)


def shards(patches, ghost_rows, courant, patch_ids, initial_load, flow_counts):
    cube, groups = lax.axis_size(CUBE), lax.axis_size(GROUPS)
    dims = cube.bit_length() - 1
    slots, side = patches.shape[0], patches.shape[1]
    records = cube * slots
    plans = capacity_classes(dims, slots)
    width = max(plans[-1])
    tab_width = dims * width + 128

    mine = jnp.concatenate([initial_load, flow_counts[:, 0, :].reshape(-1)])
    mine = jnp.pad(mine, (0, 128 - slots - mine.shape[0]))
    mine = jnp.concatenate([mine, patch_ids])
    everyone = lax.all_gather(mine, (GROUPS, CUBE))
    ids = everyone[:, 128 - slots :].reshape(groups, records)

    vmem, smem = pl.BlockSpec(memory_space=pltpu.VMEM), pl.BlockSpec(memory_space=pltpu.SMEM)
    tab, word, final_ids, imbalance = pl.pallas_call(
        functools.partial(plan_kernel, groups, cube, dims, slots, plans, width),
        out_shape=(
            jax.ShapeDtypeStruct((8, tab_width), jnp.int32),
            jax.ShapeDtypeStruct((8,), jnp.int32),
            jax.ShapeDtypeStruct((1, 128), jnp.int32),
            jax.ShapeDtypeStruct((1, 128), jnp.float32),
        ),
        in_specs=[vmem, vmem],
        out_specs=(vmem, smem, vmem, vmem),
    )(everyone, ids)
    advected = advect(patches, ghost_rows, courant)

    def mover(k):
        caps = plans[k]
        block = lambda n: pltpu.VMEM((n, side, side), jnp.float32)
        return pl.pallas_call(
            functools.partial(move_kernel, caps, slots, width),
            out_shape=jax.ShapeDtypeStruct((slots, side, side), jnp.float32),
            in_specs=[smem, smem, pl.BlockSpec(memory_space=pl.ANY)],
            out_specs=vmem,
            scratch_shapes=[block(slots + sum(caps))]
            + [block(max(caps))] + [block(n) for n in caps]
            + [pltpu.SemaphoreType.DMA((dims,)), pltpu.SemaphoreType.DMA((dims,)), pltpu.SemaphoreType.DMA],
            compiler_params=pltpu.CompilerParams(
                collective_id=k, has_side_effects=True, vmem_limit_bytes=62 * 2**20
            ),
        )

    placed = lax.switch(word[0], [mover(k) for k in range(len(plans))], tab, word, advected)
    return placed, final_ids[0, :slots], imbalance[0, :SWEEPS]


def solution(mesh):
    in_specs = (
        P((GROUPS, CUBE), None, None),
        P((GROUPS, CUBE), None, None),
        P((GROUPS, CUBE), None),
        P((GROUPS, CUBE)),
        P((GROUPS, CUBE)),
        P(None, (GROUPS, CUBE), None),
    )
    out_specs = (P((GROUPS, CUBE), None, None), P((GROUPS, CUBE)), P(GROUPS))
    return jax.shard_map(shards, mesh=mesh, in_specs=in_specs, out_specs=out_specs, check_vma=False)
```

```python
import functools

import jax
import jax.numpy as jnp
from jax import lax
from jax.experimental import pallas as pl
from jax.experimental.pallas import tpu as pltpu
from jax.sharding import PartitionSpec as P

SWEEPS = 3
CUBE = "cube"
GROUPS = "groups"


CAPACITIES = (
    (10, 6, 5, 5),
    (10, 7, 8, 4),
    (10, 7, 6, 6),
    (12, 9, 6, 4),
    (10, 8, 9, 5),
    (11, 9, 7, 6),
    (11, 9, 8, 7),
    (12, 10, 10, 8),
    (16, 14, 12, 10),
)


def capacity_classes(dims, slots):
    full = [slots * 2 ** min(b, dims - 1 - b) for b in range(dims)]
    plans = [tuple(min(f, row[min(b, len(row) - 1)]) for b, f in enumerate(full)) for row in CAPACITIES]
    return plans + [tuple(full)]


def partner_rows(value, bit, index):
    size = value.shape[0]
    up = pltpu.roll(value, 2**bit, axis=0)
    down = pltpu.roll(value, size - 2**bit, axis=0)
    return jnp.where(((index >> bit) & 1) == 1, up, down)


def track(meta, cube, dims, slots):
    records = cube * slots
    wide = (cube, 128)
    row = lax.broadcasted_iota(jnp.int32, wide, 0)
    device = lax.broadcasted_iota(jnp.int32, (cube, records), 0)
    index = lax.broadcasted_iota(jnp.int32, (1, records), 1)
    origin, start = index // slots, index % slots
    load = jnp.broadcast_to(meta[:, 0:1], wide)

    def look_up(where, column):
        picked = jnp.where(device == where, jnp.broadcast_to(column[:, 0:1], device.shape), 0)
        return jnp.sum(picked, axis=0, keepdims=True)

    occupied = start < look_up(origin, load)
    at, pos = origin, start
    peaks = []
    for sweep in range(SWEEPS):
        for bit in range(dims):
            column = 1 + sweep * dims + bit
            count = jnp.broadcast_to(meta[:, column : column + 1], wide)
            free = load - count
            shift = partner_rows(free, bit, row) - free
            moves = occupied & (pos >= look_up(at, free))
            pos = pos + jnp.where(moves, look_up(at, shift), 0)
            at = jnp.where(moves, at ^ (2**bit), at)
            load = free + partner_rows(count, bit, row)
        peaks.append(jnp.max(load))
    total = jnp.sum(meta[:, 0:1].astype(jnp.float32))
    crossing = []
    for bit in range(dims):
        low = 2**bit - 1
        current = (at & low) | (origin & ~low)
        mover = occupied & ((((origin ^ at) >> bit) & 1) == 1)
        current = jnp.where(mover, current, -1)
        crossing.append((current, (device == current).astype(jnp.float32)))
    needs = [jnp.max(jnp.sum(hot, axis=1, keepdims=True)).astype(jnp.int32) for _, hot in crossing]
    return occupied, at, pos, load, start, peaks, total, crossing, needs


def plan_kernel(groups, cube, dims, slots, plans, width, meta_ref, ids_ref, tab_ref, word_ref, ids_out_ref, imb_ref):
    me, group = lax.axis_index(CUBE), lax.axis_index(GROUPS)
    records = cube * slots
    meta = meta_ref[pl.ds(pl.multiple_of(group * cube, cube), cube), :]
    occupied, at, pos, load, start, peaks, total, crossing, needs = track(meta, cube, dims, slots)
    for other in range(1, groups):
        there = lax.rem(group + other, groups)
        block = meta_ref[pl.ds(pl.multiple_of(there * cube, cube), cube), :]
        more = track(block, cube, dims, slots)[-1]
        needs = [jnp.maximum(a, b) for a, b in zip(needs, more)]
    choice = jnp.int32(len(plans) - 1)
    for k in reversed(range(len(plans) - 1)):
        fits = needs[0] <= plans[k][0]
        for b in range(1, dims):
            fits = fits & (needs[b] <= plans[k][b])
        choice = jnp.where(fits, k, choice)
    bases = []
    for b in range(dims):
        base = jnp.int32(0)
        for k, plan in enumerate(plans):
            base = jnp.where(choice == k, slots + sum(plan[:b]), base)
        bases.append(base)

    hot = jnp.concatenate([h for _, h in crossing], axis=0).astype(jnp.bfloat16)
    before = lax.broadcasted_iota(jnp.int32, (records, records), 0) < lax.broadcasted_iota(
        jnp.int32, (records, records), 1
    )
    ranks = jnp.dot(hot, before.astype(jnp.bfloat16), preferred_element_type=jnp.float32)
    slot = start
    rows, keys = [], []
    column = lax.broadcasted_iota(jnp.int32, (width, records), 0)
    for b in range(dims):
        current, own = crossing[b]
        rank = jnp.sum(own * ranks[b * cube : (b + 1) * cube], axis=0, keepdims=True).astype(jnp.int32)
        rows.append(slot)
        keys.append((column == jnp.where(current == me, rank, -1)).astype(jnp.float32))
        slot = jnp.where(current >= 0, bases[b] + rank, slot)
    rows += [slot, ids_ref[pl.ds(group, 1), :]]
    column = lax.broadcasted_iota(jnp.int32, (128, records), 0)
    keys.append((column == jnp.where(occupied & (at == me), pos, -1)).astype(jnp.float32))
    rows += [jnp.zeros((1, records), jnp.int32)] * (8 - len(rows))
    left = jnp.concatenate(rows, axis=0).astype(jnp.float32)
    right = jnp.concatenate(keys, axis=0)
    table = lax.dot_general(
        left, right, (((1,), (1,)), ((), ())),
        precision=lax.Precision.HIGHEST, preferred_element_type=jnp.float32,
    ).astype(jnp.int32)
    tab_ref[...] = table
    mine = lax.broadcasted_iota(jnp.int32, load.shape, 0) == me
    held = jnp.sum(jnp.where(mine, load, 0), axis=0, keepdims=True)
    lane = lax.broadcasted_iota(jnp.int32, (1, 128), 1)
    ids_out_ref[...] = jnp.where(lane < held, table[dims + 1 : dims + 2, dims * width : dims * width + 128], -1)
    word_ref[0] = choice
    word_ref[1] = jnp.max(held)
    peak = jnp.zeros((1, 128), jnp.float32)
    for sweep in range(SWEEPS):
        peak = jnp.where(lane == sweep, peaks[sweep].astype(jnp.float32), peak)
    imb_ref[...] = peak * float(cube) / total


def move_kernel(caps, slots, width, tab_ref, word_ref, adv_ref, out_ref, main, *scratch):
    dims = len(caps)
    outbox, recvs = scratch[0], scratch[1 : 1 + dims]
    send_sem, recv_sem, load_sem = scratch[1 + dims :]
    me = lax.axis_index(CUBE)
    partners = [me + 2**b - 2 * 2**b * ((me // 2**b) % 2) for b in range(dims)]
    fetch = pltpu.make_async_copy(adv_ref, main.at[pl.ds(0, slots)], load_sem)
    fetch.start()
    barrier = pltpu.get_barrier_semaphore()
    for p in partners:
        pl.semaphore_signal(barrier, inc=1, device_id={CUBE: p}, device_id_type=pl.DeviceIdType.MESH)
    pl.semaphore_wait(barrier, dims)
    fetch.wait()
    base = slots
    for b in range(dims):
        send, recv = outbox.at[pl.ds(0, caps[b])], recvs[b]

        def pack(j, carry):
            send[j] = main[tab_ref[b, b * width + j]]
            return carry

        lax.fori_loop(0, caps[b], pack, 0)
        copy = pltpu.make_async_remote_copy(
            src_ref=send, dst_ref=recv, send_sem=send_sem.at[b], recv_sem=recv_sem.at[b],
            device_id={CUBE: partners[b]}, device_id_type=pl.DeviceIdType.MESH,
        )
        copy.start()
        copy.wait()

        def keep(j, carry):
            main[base + j] = recv[j]
            return carry

        lax.fori_loop(0, caps[b], keep, 0)
        base += caps[b]

    held = word_ref[1]

    def place(j, carry):
        out_ref[j] = jnp.where(j < held, main[tab_ref[dims, dims * width + j]], 0.0)
        return carry

    lax.fori_loop(0, slots, place, 0)


def advect(field, ghosts, along_x, along_y):
    row = lax.broadcasted_iota(jnp.int32, field.shape, 0)
    lane = lax.broadcasted_iota(jnp.int32, field.shape, 1)
    left = jnp.broadcast_to(ghosts[1:2], field.shape)
    left = jnp.sum(jnp.where(row == lane, left, 0.0), axis=1, keepdims=True)
    western = jnp.where(lane == 0, jnp.broadcast_to(left, field.shape), pltpu.roll(field, 1, axis=1))
    northern = jnp.where(row == 0, jnp.broadcast_to(ghosts[0:1], field.shape), pltpu.roll(field, 1, axis=0))
    return field - along_x * (field - western) - along_y * (field - northern)


def gather_kernel(total, cube, mine_ref, patch_ref, ghost_ref, courant_ref, all_ref, adv_ref, box, send_sem, recv_sem):
    slots = patch_ref.shape[0]
    me = lax.axis_index(GROUPS) * cube + lax.axis_index(CUBE)
    half = slots // 2

    def peer(k):
        there = lax.rem(me + k, total)
        return (there // cube, lax.rem(there, cube))

    def copy(k):
        return pltpu.make_async_remote_copy(
            src_ref=mine_ref, dst_ref=box.at[k], send_sem=send_sem.at[k], recv_sem=recv_sem.at[k],
            device_id=peer(k), device_id_type=pl.DeviceIdType.MESH,
        )

    def greet(k, carry):
        pl.semaphore_signal(barrier, inc=1, device_id=peer(k), device_id_type=pl.DeviceIdType.MESH)
        return carry

    def launch(k, carry):
        copy(k).start()
        return carry

    def collect(k, carry):
        copy(k).wait()
        all_ref[lax.rem(me + total - k, total)] = box[k]
        return carry

    def step(j, carry):
        adv_ref[j] = advect(patch_ref[j], ghost_ref[j], courant_ref[2 * j], courant_ref[2 * j + 1])
        return carry

    barrier = pltpu.get_barrier_semaphore()
    lax.fori_loop(1, total, greet, 0)
    all_ref[me] = mine_ref[...]
    lax.fori_loop(0, half, step, 0)
    pl.semaphore_wait(barrier, total - 1)
    lax.fori_loop(1, total, launch, 0)
    lax.fori_loop(half, slots, step, 0)
    lax.fori_loop(1, total, collect, 0)


def shards(patches, ghost_rows, courant, patch_ids, initial_load, flow_counts):
    cube, groups = lax.axis_size(CUBE), lax.axis_size(GROUPS)
    dims = cube.bit_length() - 1
    slots, side = patches.shape[0], patches.shape[1]
    records = cube * slots
    plans = capacity_classes(dims, slots)
    width = max(plans[-1])
    tab_width = dims * width + 128

    mine = jnp.concatenate([initial_load, flow_counts[:, 0, :].reshape(-1)])
    mine = jnp.pad(mine, (0, 128 - slots - mine.shape[0]))
    mine = jnp.concatenate([mine, patch_ids])
    total = groups * cube
    vmem, smem = pl.BlockSpec(memory_space=pltpu.VMEM), pl.BlockSpec(memory_space=pltpu.SMEM)
    everyone, advected = pl.pallas_call(
        functools.partial(gather_kernel, total, cube),
        out_shape=(
            jax.ShapeDtypeStruct((total, 1, 128), jnp.int32),
            jax.ShapeDtypeStruct(patches.shape, jnp.float32),
        ),
        in_specs=[vmem, vmem, vmem, smem],
        out_specs=(vmem, vmem),
        scratch_shapes=[
            pltpu.VMEM((total, 1, 128), jnp.int32),
            pltpu.SemaphoreType.DMA((total,)),
            pltpu.SemaphoreType.DMA((total,)),
        ],
        compiler_params=pltpu.CompilerParams(collective_id=0, has_side_effects=True),
    )(mine[None], patches, ghost_rows, courant.reshape(-1))
    everyone = everyone[:, 0]
    ids = everyone[:, 128 - slots :].reshape(groups, records)

    tab, word, final_ids, imbalance = pl.pallas_call(
        functools.partial(plan_kernel, groups, cube, dims, slots, plans, width),
        out_shape=(
            jax.ShapeDtypeStruct((8, tab_width), jnp.int32),
            jax.ShapeDtypeStruct((8,), jnp.int32),
            jax.ShapeDtypeStruct((1, 128), jnp.int32),
            jax.ShapeDtypeStruct((1, 128), jnp.float32),
        ),
        in_specs=[vmem, vmem],
        out_specs=(vmem, smem, vmem, vmem),
    )(everyone, ids)

    def mover(k):
        caps = plans[k]
        block = lambda n: pltpu.VMEM((n, side, side), jnp.float32)
        return pl.pallas_call(
            functools.partial(move_kernel, caps, slots, width),
            out_shape=jax.ShapeDtypeStruct((slots, side, side), jnp.float32),
            in_specs=[smem, smem, pl.BlockSpec(memory_space=pl.ANY)],
            out_specs=vmem,
            scratch_shapes=[block(slots + sum(caps))]
            + [block(max(caps))] + [block(n) for n in caps]
            + [pltpu.SemaphoreType.DMA((dims,)), pltpu.SemaphoreType.DMA((dims,)), pltpu.SemaphoreType.DMA],
            compiler_params=pltpu.CompilerParams(
                collective_id=k + 1, has_side_effects=True, vmem_limit_bytes=62 * 2**20
            ),
        )

    placed = lax.switch(word[0], [mover(k) for k in range(len(plans))], tab, word, advected)
    return placed, final_ids[0, :slots], imbalance[0, :SWEEPS]


def solution(mesh):
    in_specs = (
        P((GROUPS, CUBE), None, None),
        P((GROUPS, CUBE), None, None),
        P((GROUPS, CUBE), None),
        P((GROUPS, CUBE)),
        P((GROUPS, CUBE)),
        P(None, (GROUPS, CUBE), None),
    )
    out_specs = (P((GROUPS, CUBE), None, None), P((GROUPS, CUBE)), P(GROUPS))
    return jax.shard_map(shards, mesh=mesh, in_specs=in_specs, out_specs=out_specs, check_vma=False)
```

```python
import functools

import jax
import jax.numpy as jnp
from jax import lax
from jax.experimental import pallas as pl
from jax.experimental.pallas import tpu as pltpu
from jax.sharding import PartitionSpec as P

SWEEPS = 3
CUBE = "cube"
GROUPS = "groups"


CAPACITIES = (
    (7, 4, 4, 2, 4, 7, 2, 4),
    (7, 4, 5, 3, 3, 6, 3, 5),
    (9, 5, 5, 3, 4, 7, 3, 6),
    (7, 4, 7, 4, 3, 6, 3, 6),
    (7, 4, 7, 4, 4, 7, 4, 7),
    (11, 6, 7, 4, 5, 9, 3, 5),
    (9, 5, 7, 4, 4, 7, 5, 9),
    (11, 6, 9, 5, 5, 9, 4, 7),
    (9, 5, 11, 6, 4, 7, 6, 11),
    (14, 14, 12, 12, 10, 14, 8, 12),
)


def orders(dims):
    first = list(range(dims))
    return [first, first[dims // 2 :] + first[: dims // 2]]


def capacity_classes(dims, slots):
    full = [min(-(-slots // 2) * 2**k, slots * 2 ** (dims - 1 - k)) for k in range(dims)]
    plans = []
    for row in CAPACITIES:
        spread = [row[min(k, len(row) - 2 + k % 2)] for k in range(2 * dims)]
        plans.append(tuple(min(full[k // 2], n) for k, n in enumerate(spread)))
    return plans + [tuple(n for n in full for _ in range(2))]


def partner_rows(value, bit, index):
    size = value.shape[0]
    up = pltpu.roll(value, 2**bit, axis=0)
    down = pltpu.roll(value, size - 2**bit, axis=0)
    return jnp.where(((index >> bit) & 1) == 1, up, down)


def track(meta, cube, dims, slots):
    records = cube * slots
    wide = (cube, 128)
    row = lax.broadcasted_iota(jnp.int32, wide, 0)
    device = lax.broadcasted_iota(jnp.int32, (cube, records), 0)
    index = lax.broadcasted_iota(jnp.int32, (1, records), 1)
    origin, start = index // slots, index % slots
    load = jnp.broadcast_to(meta[:, 0:1], wide)

    def look_up(where, column):
        picked = jnp.where(device == where, jnp.broadcast_to(column[:, 0:1], device.shape), 0)
        return jnp.sum(picked, axis=0, keepdims=True)

    occupied = start < look_up(origin, load)
    at, pos = origin, start
    peaks = []
    for sweep in range(SWEEPS):
        for bit in range(dims):
            column = 1 + sweep * dims + bit
            count = jnp.broadcast_to(meta[:, column : column + 1], wide)
            free = load - count
            shift = partner_rows(free, bit, row) - free
            moves = occupied & (pos >= look_up(at, free))
            pos = pos + jnp.where(moves, look_up(at, shift), 0)
            at = jnp.where(moves, at ^ (2**bit), at)
            load = free + partner_rows(count, bit, row)
        peaks.append(jnp.max(load))
    total = jnp.sum(meta[:, 0:1].astype(jnp.float32))
    crossing = []
    for k in range(2 * dims):
        order = orders(dims)[k % 2]
        bit, done = order[k // 2], sum(2**b for b in order[: k // 2])
        current = (at & done) | (origin & ~done)
        mover = occupied & (start % 2 == k % 2) & ((((origin ^ at) >> bit) & 1) == 1)
        current = jnp.where(mover, current, -1)
        crossing.append((current, (device == current).astype(jnp.float32)))
    needs = [jnp.max(jnp.sum(hot, axis=1, keepdims=True)).astype(jnp.int32) for _, hot in crossing]
    return occupied, at, pos, load, start, peaks, total, crossing, needs


def plan_kernel(groups, cube, dims, slots, plans, width, meta_ref, ids_ref, tab_ref, word_ref, ids_out_ref, imb_ref):
    me, group = lax.axis_index(CUBE), lax.axis_index(GROUPS)
    records = cube * slots
    meta = meta_ref[pl.ds(pl.multiple_of(group * cube, cube), cube), :]
    occupied, at, pos, load, start, peaks, total, crossing, needs = track(meta, cube, dims, slots)
    for other in range(1, groups):
        there = lax.rem(group + other, groups)
        block = meta_ref[pl.ds(pl.multiple_of(there * cube, cube), cube), :]
        more = track(block, cube, dims, slots)[-1]
        needs = [jnp.maximum(a, b) for a, b in zip(needs, more)]
    choice = jnp.int32(len(plans) - 1)
    for k in reversed(range(len(plans) - 1)):
        fits = needs[0] <= plans[k][0]
        for b in range(1, 2 * dims):
            fits = fits & (needs[b] <= plans[k][b])
        choice = jnp.where(fits, k, choice)
    bases = []
    for b in range(2 * dims):
        base = jnp.int32(0)
        for k, plan in enumerate(plans):
            base = jnp.where(choice == k, slots + sum(plan[:b]), base)
        bases.append(base)

    hot = jnp.concatenate([h for _, h in crossing], axis=0).astype(jnp.bfloat16)
    before = lax.broadcasted_iota(jnp.int32, (records, records), 0) < lax.broadcasted_iota(
        jnp.int32, (records, records), 1
    )
    ranks = jnp.dot(hot, before.astype(jnp.bfloat16), preferred_element_type=jnp.float32)
    slot = start
    rows, keys = [], []
    column = lax.broadcasted_iota(jnp.int32, (width, records), 0)
    for b in range(2 * dims):
        current, own = crossing[b]
        rank = jnp.sum(own * ranks[b * cube : (b + 1) * cube], axis=0, keepdims=True).astype(jnp.int32)
        rows += [slot] if b % 2 == 0 else []
        keys.append((column == jnp.where(current == me, rank, -1)).astype(jnp.float32))
        slot = jnp.where(current >= 0, bases[b] + rank, slot)
    rows += [slot, ids_ref[pl.ds(group, 1), :]]
    column = lax.broadcasted_iota(jnp.int32, (128, records), 0)
    keys.append((column == jnp.where(occupied & (at == me), pos, -1)).astype(jnp.float32))
    rows += [jnp.zeros((1, records), jnp.int32)] * (8 - len(rows))
    left = jnp.concatenate(rows, axis=0).astype(jnp.float32)
    right = jnp.concatenate(keys, axis=0)
    table = lax.dot_general(
        left, right, (((1,), (1,)), ((), ())),
        precision=lax.Precision.HIGHEST, preferred_element_type=jnp.float32,
    ).astype(jnp.int32)
    tab_ref[...] = table
    mine = lax.broadcasted_iota(jnp.int32, load.shape, 0) == me
    held = jnp.sum(jnp.where(mine, load, 0), axis=0, keepdims=True)
    lane = lax.broadcasted_iota(jnp.int32, (1, 128), 1)
    ids_out_ref[...] = jnp.where(lane < held, table[dims + 1 : dims + 2, 2 * dims * width : 2 * dims * width + 128], -1)
    word_ref[0] = choice
    word_ref[1] = jnp.max(held)
    peak = jnp.zeros((1, 128), jnp.float32)
    for sweep in range(SWEEPS):
        peak = jnp.where(lane == sweep, peaks[sweep].astype(jnp.float32), peak)
    imb_ref[...] = peak * float(cube) / total


def move_kernel(caps, slots, width, tab_ref, word_ref, adv_ref, out_ref, main, *scratch):
    count = len(caps)
    dims = count // 2
    outbox, recvs = scratch[:2], scratch[2 : 2 + count]
    send_sem, recv_sem, load_sem = scratch[2 + count :]
    me = lax.axis_index(CUBE)
    partners = [me + 2**b - 2 * 2**b * ((me // 2**b) % 2) for b in range(dims)]
    fetch = pltpu.make_async_copy(adv_ref, main.at[pl.ds(0, slots)], load_sem)
    fetch.start()
    barrier = pltpu.get_barrier_semaphore()
    for p in partners:
        pl.semaphore_signal(barrier, inc=1, device_id={CUBE: p}, device_id_type=pl.DeviceIdType.MESH)
    pl.semaphore_wait(barrier, dims)
    fetch.wait()
    base = slots
    for k in range(dims):
        copies = []
        for half in (1, 0):
            b = 2 * k + half
            send = outbox[half].at[pl.ds(0, caps[b])]

            def pack(j, carry):
                send[j] = main[tab_ref[k, b * width + j]]
                return carry

            lax.fori_loop(0, caps[b], pack, 0)
            copy = pltpu.make_async_remote_copy(
                src_ref=send, dst_ref=recvs[b], send_sem=send_sem.at[b], recv_sem=recv_sem.at[b],
                device_id={CUBE: partners[orders(dims)[half][k]]}, device_id_type=pl.DeviceIdType.MESH,
            )
            copy.start()
            copies.insert(0, copy)
        for half in (0, 1):
            b = 2 * k + half
            copies[half].wait()
            if k == dims - 1:
                continue
            recv = recvs[b]

            def keep(j, carry):
                main[base + j] = recv[j]
                return carry

            lax.fori_loop(0, caps[b], keep, 0)
            base += caps[b]

    held = word_ref[1]
    even, odd = recvs[count - 2], recvs[count - 1]
    even_base, odd_base = base, base + caps[count - 2]

    def place(j, carry):
        s = tab_ref[dims, count * width + j]
        value = main[jnp.minimum(s, even_base - 1)]
        late = even[jnp.clip(s - even_base, 0, caps[count - 2] - 1)]
        value = jnp.where(s >= even_base, late, value)
        late = odd[jnp.clip(s - odd_base, 0, caps[count - 1] - 1)]
        value = jnp.where(s >= odd_base, late, value)
        out_ref[j] = jnp.where(j < held, value, 0.0)
        return carry

    lax.fori_loop(0, slots, place, 0)


def advect(field, ghosts, along_x, along_y):
    row = lax.broadcasted_iota(jnp.int32, field.shape, 0)
    lane = lax.broadcasted_iota(jnp.int32, field.shape, 1)
    left = jnp.broadcast_to(ghosts[1:2], field.shape)
    left = jnp.sum(jnp.where(row == lane, left, 0.0), axis=1, keepdims=True)
    western = jnp.where(lane == 0, jnp.broadcast_to(left, field.shape), pltpu.roll(field, 1, axis=1))
    northern = jnp.where(row == 0, jnp.broadcast_to(ghosts[0:1], field.shape), pltpu.roll(field, 1, axis=0))
    return field - along_x * (field - western) - along_y * (field - northern)


def gather_kernel(total, cube, mine_ref, patch_ref, ghost_ref, courant_ref, all_ref, adv_ref, box, send_sem, recv_sem):
    slots = patch_ref.shape[0]
    me = lax.axis_index(GROUPS) * cube + lax.axis_index(CUBE)
    half = slots // 2

    def peer(k):
        there = lax.rem(me + k, total)
        return (there // cube, lax.rem(there, cube))

    def copy(k):
        return pltpu.make_async_remote_copy(
            src_ref=mine_ref, dst_ref=box.at[k], send_sem=send_sem.at[k], recv_sem=recv_sem.at[k],
            device_id=peer(k), device_id_type=pl.DeviceIdType.MESH,
        )

    def greet(k, carry):
        pl.semaphore_signal(barrier, inc=1, device_id=peer(k), device_id_type=pl.DeviceIdType.MESH)
        return carry

    def launch(k, carry):
        copy(k).start()
        return carry

    def collect(k, carry):
        copy(k).wait()
        all_ref[lax.rem(me + total - k, total)] = box[k]
        return carry

    def step(j, carry):
        adv_ref[j] = advect(patch_ref[j], ghost_ref[j], courant_ref[2 * j], courant_ref[2 * j + 1])
        return carry

    barrier = pltpu.get_barrier_semaphore()
    lax.fori_loop(1, total, greet, 0)
    all_ref[me] = mine_ref[...]
    lax.fori_loop(0, half, step, 0)
    pl.semaphore_wait(barrier, total - 1)
    lax.fori_loop(1, total, launch, 0)
    lax.fori_loop(half, slots, step, 0)
    lax.fori_loop(1, total, collect, 0)


def shards(patches, ghost_rows, courant, patch_ids, initial_load, flow_counts):
    cube, groups = lax.axis_size(CUBE), lax.axis_size(GROUPS)
    dims = cube.bit_length() - 1
    slots, side = patches.shape[0], patches.shape[1]
    records = cube * slots
    plans = capacity_classes(dims, slots)
    width = max(plans[-1])
    tab_width = 2 * dims * width + 128

    mine = jnp.concatenate([initial_load, flow_counts[:, 0, :].reshape(-1)])
    mine = jnp.pad(mine, (0, 128 - slots - mine.shape[0]))
    mine = jnp.concatenate([mine, patch_ids])
    total = groups * cube
    vmem, smem = pl.BlockSpec(memory_space=pltpu.VMEM), pl.BlockSpec(memory_space=pltpu.SMEM)
    everyone, advected = pl.pallas_call(
        functools.partial(gather_kernel, total, cube),
        out_shape=(
            jax.ShapeDtypeStruct((total, 1, 128), jnp.int32),
            jax.ShapeDtypeStruct(patches.shape, jnp.float32),
        ),
        in_specs=[vmem, vmem, vmem, smem],
        out_specs=(vmem, vmem),
        scratch_shapes=[
            pltpu.VMEM((total, 1, 128), jnp.int32),
            pltpu.SemaphoreType.DMA((total,)),
            pltpu.SemaphoreType.DMA((total,)),
        ],
        compiler_params=pltpu.CompilerParams(collective_id=0, has_side_effects=True),
    )(mine[None], patches, ghost_rows, courant.reshape(-1))
    everyone = everyone[:, 0]
    ids = everyone[:, 128 - slots :].reshape(groups, records)

    tab, word, final_ids, imbalance = pl.pallas_call(
        functools.partial(plan_kernel, groups, cube, dims, slots, plans, width),
        out_shape=(
            jax.ShapeDtypeStruct((8, tab_width), jnp.int32),
            jax.ShapeDtypeStruct((8,), jnp.int32),
            jax.ShapeDtypeStruct((1, 128), jnp.int32),
            jax.ShapeDtypeStruct((1, 128), jnp.float32),
        ),
        in_specs=[vmem, vmem],
        out_specs=(vmem, smem, vmem, vmem),
    )(everyone, ids)

    def mover(k):
        caps = plans[k]
        block = lambda n: pltpu.VMEM((n, side, side), jnp.float32)
        return pl.pallas_call(
            functools.partial(move_kernel, caps, slots, width),
            out_shape=jax.ShapeDtypeStruct((slots, side, side), jnp.float32),
            in_specs=[smem, smem, pl.BlockSpec(memory_space=pl.ANY)],
            out_specs=vmem,
            scratch_shapes=[block(slots + sum(caps[:-2]))]
            + [block(max(caps[0::2])), block(max(caps[1::2]))] + [block(n) for n in caps]
            + [pltpu.SemaphoreType.DMA((2 * dims,)), pltpu.SemaphoreType.DMA((2 * dims,)), pltpu.SemaphoreType.DMA],
            compiler_params=pltpu.CompilerParams(
                collective_id=k + 1, has_side_effects=True, vmem_limit_bytes=62 * 2**20
            ),
        )

    placed = lax.switch(word[0], [mover(k) for k in range(len(plans))], tab, word, advected)
    return placed, final_ids[0, :slots], imbalance[0, :SWEEPS]


def solution(mesh):
    in_specs = (
        P((GROUPS, CUBE), None, None),
        P((GROUPS, CUBE), None, None),
        P((GROUPS, CUBE), None),
        P((GROUPS, CUBE)),
        P((GROUPS, CUBE)),
        P(None, (GROUPS, CUBE), None),
    )
    out_specs = (P((GROUPS, CUBE), None, None), P((GROUPS, CUBE)), P(GROUPS))
    return jax.shard_map(shards, mesh=mesh, in_specs=in_specs, out_specs=out_specs, check_vma=False)
```
